32 devices in a mesh: band: 2 (over core), lane: 16 (over z, y, x).
Axes of the slice: x: 2, y: 2, z: 4, core: 2. Of those that a mesh axis runs over, the one named last changes fastest.
Arguments:
- load_terms: float32 [128, 1024, 128], P('band', 'lane'), may hold values from -6 to 6
- start_values: float32 [128, 1024, 128], P('band', 'lane'), may hold values from -6 to 6
- reaction_rate: float32 [128, 1024, 128], P('band', 'lane'), may hold values from 0.1 to 0.9
Outputs:
- solution: float32 [128, 1024, 128], P('band', 'lane')
The draws below stay inside these ranges and needn't reach their ends.
All inputs are finite; a program needn't handle non-finite values.
Results may differ from the reference program's by a relative error of at most 0.0003.
Values sent between devices are 32-bit elements.
A program may use at most 64 MiB of HBM per device.

```python
import jax
import jax.numpy as jnp
from jax import lax

LAYERS = 128
RATIO = 4
BEFORE = 3
AFTER = 2
INNER = 13
GRID_Y = 128
GRID_X = 1024


def steps_of(stream_key, dims, cuts, smallest, high):
    gain = 1.0
    for position, blocks in cuts:
        steps = jax.random.uniform(jax.random.fold_in(jax.random.fold_in(stream_key, 6), position), (blocks,), jnp.float32, smallest / len(cuts), high / len(cuts))
        gain = gain * jnp.repeat(jnp.exp(steps), dims[position] // blocks).reshape((-1,) + (1,) * (len(dims) - 1 - position))
    return gain


def noise(stream_key, shape, width, limit, cuts=(), dtype=jnp.bfloat16):
    values = jax.random.normal(stream_key, shape, jnp.float32) * width
    if len(cuts) > 0:
        values = steps_of(stream_key, shape, cuts, -0.22, 0.18) * values
    return jnp.clip(values, min=-limit, max=limit).astype(dtype)


def setup_inputs(seed: int = 0) -> dict:
    seeds = jax.random.split(jax.random.key(seed), 4)
    return {
        "load_terms": noise(seeds[0], (GRID_Y, GRID_X, LAYERS), 1.0, 6.0, ((0, 2), (1, 16)), jnp.float32),
        "start_values": noise(seeds[1], (GRID_Y, GRID_X, LAYERS), 1.0, 6.0, ((0, 2), (1, 16)), jnp.float32),
        "reaction_rate": jnp.clip(0.1 + 0.79999997 * jax.random.uniform(seeds[2], (GRID_Y, GRID_X, LAYERS), jnp.float32) ** steps_of(seeds[2], (GRID_Y, GRID_X, LAYERS), ((0, 2), (1, 16)), -0.2, 0.2), 0.1, 0.9),
    }


def cross_sum(padded):
    inner_y, inner_x = padded.shape[0] - 2, padded.shape[1] - 2
    middle_rows = lax.slice_in_dim(padded, 1, 1 + inner_y, axis=0)
    middle_columns = lax.slice_in_dim(padded, 1, 1 + inner_x, axis=1)
    return (lax.slice_in_dim(middle_columns, 0, inner_y, axis=0) + lax.slice_in_dim(middle_columns, 2, 2 + inner_y, axis=0)
            + lax.slice_in_dim(middle_rows, 0, inner_x, axis=1) + lax.slice_in_dim(middle_rows, 2, 2 + inner_x, axis=1))


def smooth_step(padded, values, load, mass_here):
    return values + 0.8 * (load + cross_sum(padded) - (4.0 + mass_here) * values) / (4.0 + mass_here)


def block_means(values):
    cut = values.reshape(values.shape[0] // RATIO, RATIO, values.shape[1] // RATIO, RATIO, values.shape[2])
    return jnp.mean(cut, axis=(1, 3))


def spread_blocks(values):
    return jnp.repeat(jnp.repeat(values, RATIO, axis=0), RATIO, axis=1)


def reference(load_terms, start_values, reaction_rate):
    values = start_values
    for sweep in range(BEFORE):
        values = smooth_step(jnp.pad(values, ((1, 1), (1, 1), (0, 0)), mode="wrap"), values, load_terms, reaction_rate)
    defect = load_terms + cross_sum(jnp.pad(values, ((1, 1), (1, 1), (0, 0)), mode="wrap")) - (4.0 + reaction_rate) * values
    coarse_load, coarse_mass = block_means(defect) * RATIO, block_means(reaction_rate) * RATIO
    coarse_values = jnp.zeros_like(coarse_load)
    for sweep in range(INNER):
        coarse_values = smooth_step(jnp.pad(coarse_values, ((1, 1), (1, 1), (0, 0)), mode="wrap"), coarse_values, coarse_load, coarse_mass)
    values = values + spread_blocks(coarse_values)
    for sweep in range(AFTER):
        values = smooth_step(jnp.pad(values, ((1, 1), (1, 1), (0, 0)), mode="wrap"), values, load_terms, reaction_rate)
    solution = values
    return solution
```

```python
import functools

import jax
import jax.numpy as jnp
from jax import lax
from jax.experimental import pallas as pl
from jax.experimental.pallas import tpu as pltpu
from jax.sharding import PartitionSpec as P

RATIO = 4
BEFORE = 3
AFTER = 2
INNER = 13
MESH = pl.DeviceIdType.MESH

PAD = 8
DEPTH = BEFORE + 1
ITEMS = DEPTH + 2 * (DEPTH - 1)
CPAD = 16


def kernel(lanes, bands, ny, nx, load_hbm, start_hbm, rate_hbm, out_hbm,
           ua, ub, fl, fw, ca, cb, c0, cw, tmp, stage,
           sx, rx, rc, csx, crx, crc, hsx, hrx, hry,
           in_sem, out_sem, xs, xr, ys, yr, cs, cr, kxs, kxr, kys, kyr, kcs, kcr, hxs, hxr, hys, hyr):
    lane, band = lax.axis_index("lane"), lax.axis_index("band")
    sides = ({"lane": lax.rem(lane + lanes - 1, lanes)}, {"lane": lax.rem(lane + 1, lanes)})
    ends = ({"band": lax.rem(band + bands - 1, bands)}, {"band": lax.rem(band + 1, bands)})
    ry, wx = ny + 2 * DEPTH, nx + 2 * PAD
    cy, cx = ny // RATIO, nx // RATIO
    cwx = cx + 2 * CPAD
    cry = cy + 2 * CPAD
    flat = lambda ref: ref.reshape(ref.shape[0] * ref.shape[1], ref.shape[2])
    fua, fub, ffl, ffw = flat(ua), flat(ub), flat(fl), flat(fw)
    fca, fcb, fc0, fcw = flat(ca), flat(cb), flat(c0), flat(cw)
    own = (pl.ds(DEPTH, ny), pl.ds(PAD, nx))

    ins = []
    for n, (src, dst) in enumerate(((start_hbm, ua), (load_hbm, fl), (rate_hbm, fw))):
        copy = pltpu.make_async_copy(src, dst.at[own[0], own[1]], in_sem.at[n])
        copy.start()
        ins.append(copy)

    barrier = pltpu.get_barrier_semaphore()
    for other in sides + ends:
        pl.semaphore_signal(barrier, inc=1, device_id=other, device_id_type=MESH)
    pl.semaphore_wait(barrier, 4)
    for copy in ins:
        copy.wait()

    def remote(src, dst, send, recv, other):
        copy = pltpu.make_async_remote_copy(src_ref=src, dst_ref=dst, send_sem=send, recv_sem=recv, device_id=other, device_id_type=MESH)
        copy.start()
        return copy

    arrays = [(fua, d) for d in range(DEPTH)] + [(ffl, d) for d in range(DEPTH - 1)] + [(ffw, d) for d in range(DEPTH - 1)]
    x_copies = []
    for side in range(2):
        for item, (ref, d) in enumerate(arrays):
            col = d if side == 0 else nx - 1 - d
            sx[side, item] = ref[pl.ds(DEPTH * wx + PAD + col, ny, stride=wx), :]
        x_copies.append(remote(sx.at[side], rx.at[1 - side], xs.at[side], xr.at[1 - side], sides[side]))

    y_copies = []
    for n, (ref, deep) in enumerate(((ua, DEPTH), (fl, DEPTH - 1), (fw, DEPTH - 1))):
        y_copies.append(remote(ref.at[pl.ds(DEPTH, deep), own[1]], ref.at[pl.ds(DEPTH + ny, deep), own[1]], ys.at[n, 0], yr.at[n, 1], ends[0]))
        y_copies.append(remote(ref.at[pl.ds(DEPTH + ny - deep, deep), own[1]], ref.at[pl.ds(DEPTH - deep, deep), own[1]], ys.at[n, 1], yr.at[n, 0], ends[1]))

    def blocks(rows_of, n):
        total = rows_of(0)
        for r in range(1, RATIO):
            total = total + rows_of(r)
        tmp[pl.ds(pl.multiple_of(n * wx, 8), nx), :] = total

    def across(n):
        base = n * wx
        total = tmp[pl.ds(base, cx, stride=RATIO), :]
        for j in range(1, RATIO):
            total = total + tmp[pl.ds(base + j, cx, stride=RATIO), :]
        return total * (1.0 / RATIO)

    def coarse_at(n):
        return pl.ds(pl.multiple_of((CPAD + n) * cwx + CPAD, 8), cx)

    def mass_row(n, carry):
        blocks(lambda r: ffw[pl.ds(pl.multiple_of((DEPTH + n * RATIO + r) * wx + PAD, 8), nx), :], n)
        fcw[coarse_at(n), :] = 0.8 / (4.0 + across(n))
        return carry

    lax.fori_loop(0, cy, mass_row, 0)

    def send_coarse(q, src):
        copies = []
        for side in range(2):
            for d in range(INNER):
                col = d if side == 0 else cx - 1 - d
                csx[side, q, d] = src[pl.ds(CPAD * cwx + CPAD + col, cy, stride=cwx), :]
            copies.append(remote(csx.at[side, q], crx.at[1 - side, q], kxs.at[side, q], kxr.at[1 - side, q], sides[side]))
        return copies

    def send_rows(q, ref):
        mine = ref.at[pl.ds(CPAD, cy), pl.ds(CPAD, cx)]
        return [
            remote(mine, ref.at[pl.ds(CPAD + cy, cy), pl.ds(CPAD, cx)], kys.at[0, q], kyr.at[1, q], ends[0]),
            remote(mine, ref.at[pl.ds(CPAD - cy, cy), pl.ds(CPAD, cx)], kys.at[1, q], kyr.at[0, q], ends[1]),
        ]

    def forward(q, side):
        return [remote(crx.at[side, q], crc.at[side, q, 1 - end], kcs.at[side, q, end], kcr.at[side, q, 1 - end], ends[end]) for end in range(2)]

    def unpack_coarse(q, dst):
        for side in range(2):
            for d in range(INNER):
                col = CPAD - 1 - d if side == 0 else CPAD + cx + d
                dst[pl.ds(CPAD * cwx + col, cy, stride=cwx), :] = crx[side, q, d]
                dst[pl.ds((CPAD - cy) * cwx + col, cy, stride=cwx), :] = crc[side, q, 0, d]
                dst[pl.ds((CPAD + cy) * cwx + col, cy, stride=cwx), :] = crc[side, q, 1, d]

    mass_x = send_coarse(0, fcw)
    mass_y = send_rows(0, cw)

    c_copies = []
    for side in range(2):
        x_copies[1 - side].wait_recv()
        for end in range(2):
            rows = pl.ds(0, 8) if end == 0 else pl.ds(ny - 8, 8)
            c_copies.append(remote(rx.at[side, :, rows], rc.at[side, 1 - end], cs.at[side, end], cr.at[side, 1 - end], ends[end]))
    for copy in y_copies:
        copy.wait()
    for side in range(2):
        for item, (ref, d) in enumerate(arrays):
            col = PAD - 1 - d if side == 0 else PAD + nx + d
            ref[pl.ds(DEPTH * wx + col, ny, stride=wx), :] = rx[side, item]
    for copy in c_copies:
        copy.wait()
    for side in range(2):
        for item, (ref, d) in enumerate(arrays):
            col = PAD - 1 - d if side == 0 else PAD + nx + d
            ref[pl.ds(col, DEPTH, stride=wx), :] = rc[side, 0, item, 8 - DEPTH:8]
            ref[pl.ds((DEPTH + ny) * wx + col, DEPTH, stride=wx), :] = rc[side, 1, item, 0:DEPTH]

    def weigh(y, carry):
        at = pl.ds(pl.multiple_of(y * wx, 8), wx)
        weight = 0.8 / (4.0 + ffw[at, :])
        ffw[at, :] = weight
        ffl[at, :] = weight * ffl[at, :]
        return carry

    lax.fori_loop(0, ry, weigh, 0)

    def sweep(src, dst, load, weight, width, first, count, low, high, put=None):
        def rows(n, carry):
            for r in range(2):
                y = first + 2 * n + r
                base = pl.multiple_of(y * width + low, 8)
                span = high - low
                here = src[pl.ds(base, span), :]
                around = (src[pl.ds(base - width, span), :] + src[pl.ds(base + width, span), :]
                          + src[pl.ds(base - 1, span), :] + src[pl.ds(base + 1, span), :])
                new = 0.2 * here + weight[pl.ds(base, span), :] * around + load[pl.ds(base, span), :]
                if put is None:
                    dst[pl.ds(base, span), :] = new
                else:
                    put(y, new)
            return carry

        lax.fori_loop(0, count // 2, rows, 0)

    sweep(fua, fub, ffl, ffw, wx, 1, ry - 2, 0, wx)
    sweep(fub, fua, ffl, ffw, wx, 2, ry - 4, 0, wx)
    sweep(fua, fub, ffl, ffw, wx, 3, ry - 6, 0, wx)

    h_copies = []
    for side in range(2):
        col = 1 if side == 0 else nx - 2
        hsx[side] = fub[pl.ds(DEPTH * wx + PAD + col, ny, stride=wx), :]
        h_copies.append(remote(hsx.at[side], hrx.at[1 - side], hxs.at[side], hxr.at[1 - side], sides[side]))
    hy_copies = [
        remote(ub.at[DEPTH + 1, own[1]], hry.at[1], hys.at[0], hyr.at[1], ends[0]),
        remote(ub.at[DEPTH + ny - 2, own[1]], hry.at[0], hys.at[1], hyr.at[0], ends[1]),
    ]

    def load_row(n, carry):
        def defect(r):
            base = pl.multiple_of((DEPTH + n * RATIO + r) * wx + PAD, 8)
            weight = ffw[pl.ds(base, nx), :]
            around = (fub[pl.ds(base - wx, nx), :] + fub[pl.ds(base + wx, nx), :]
                      + fub[pl.ds(base - 1, nx), :] + fub[pl.ds(base + 1, nx), :])
            return around + (ffl[pl.ds(base, nx), :] - 0.8 * fub[pl.ds(base, nx), :]) / weight

        blocks(defect, n)
        fc0[coarse_at(n), :] = fcw[coarse_at(n), :] * across(n)
        return carry

    lax.fori_loop(0, cy, load_row, 0)

    load_x = send_coarse(1, fc0)
    load_y = send_rows(1, c0)
    forwards = []
    for side in range(2):
        mass_x[1 - side].wait_recv()
        forwards += forward(0, side)
    for copy in mass_y + forwards:
        copy.wait()
    unpack_coarse(0, fcw)
    forwards = []
    for side in range(2):
        load_x[1 - side].wait_recv()
        forwards += forward(1, side)
    for copy in load_y + forwards:
        copy.wait()
    unpack_coarse(1, fc0)

    now, later = fc0, fca
    for t in range(2, INNER + 1):
        reach = INNER + 1 - t
        low = (CPAD - reach) // 8 * 8
        high = -((-(CPAD + cx + reach)) // 8) * 8
        sweep(now, later, fc0, fcw, cwx, CPAD - reach, cy + 2 * reach, low, high)
        now, later = later, (fcb if t % 2 == 0 else fca)

    for copy in h_copies:
        copy.wait_recv()
    for copy in hy_copies:
        copy.wait()
    for side in range(2):
        col = PAD - 2 if side == 0 else PAD + nx + 1
        fub[pl.ds(DEPTH * wx + col, ny, stride=wx), :] = hrx[side]
    ub[DEPTH - 2, own[1]] = hry[0]
    ub[DEPTH + ny + 1, own[1]] = hry[1]
    count = wx // RATIO
    for n in range(cy + 2):
        row = now[pl.ds((CPAD - 1 + n) * cwx + CPAD - PAD // RATIO, count), :]
        for j in range(RATIO):
            tmp[pl.ds(n * wx + j, count, stride=RATIO), :] = row

    def correct(n, carry):
        extra = tmp[pl.ds(pl.multiple_of(n * wx, 8), wx), :]
        for r in range(RATIO):
            at = pl.ds(pl.multiple_of((n * RATIO + r) * wx, 8), wx)
            fub[at, :] = fub[at, :] + extra
        return carry

    lax.fori_loop(0, cy + 2, correct, 0)
    sweep(fub, fua, ffl, ffw, wx, DEPTH - 1, ny + 2, 0, wx)

    def put(y, new):
        stage[y - DEPTH] = new

    pieces = 4
    outs = []
    for piece in range(pieces):
        part = ny // pieces
        sweep(fua, None, ffl, ffw, wx, DEPTH + piece * part, part, PAD, PAD + nx, put)
        at = pl.ds(piece * part, part)
        copy = pltpu.make_async_copy(stage.at[at], out_hbm.at[at], out_sem.at[piece])
        copy.start()
        outs.append(copy)
    for copy in x_copies + mass_x + load_x + h_copies:
        copy.wait_send()
    for copy in outs:
        copy.wait()


def shards(lanes, bands, load_terms, start_values, reaction_rate):
    ny, nx, layers = load_terms.shape
    f32 = jnp.float32
    ry, wx = ny + 2 * DEPTH, nx + 2 * PAD
    cy, cx = ny // RATIO, nx // RATIO
    assert ny % 8 == 0 and nx % 8 == 0 and INNER <= min(cy, cx) <= CPAD and layers == 128
    fine = pltpu.VMEM((ry, wx, layers), f32)
    coarse = pltpu.VMEM((cy + 2 * CPAD, cx + 2 * CPAD, layers), f32)
    dma = pltpu.SemaphoreType.DMA
    return pl.pallas_call(
        functools.partial(kernel, lanes, bands, ny, nx),
        out_shape=jax.ShapeDtypeStruct(load_terms.shape, f32),
        in_specs=[pl.BlockSpec(memory_space=pl.ANY)] * 3,
        out_specs=pl.BlockSpec(memory_space=pl.ANY),
        scratch_shapes=[
            fine, fine, fine, fine, coarse, coarse, coarse, coarse,
            pltpu.VMEM(((cy + 2) * wx, layers), f32),
            pltpu.VMEM((ny, nx, layers), f32),
            pltpu.VMEM((2, ITEMS, ny, layers), f32),
            pltpu.VMEM((2, ITEMS, ny, layers), f32),
            pltpu.VMEM((2, 2, ITEMS, 8, layers), f32),
            pltpu.VMEM((2, 2, INNER, cy, layers), f32),
            pltpu.VMEM((2, 2, INNER, cy, layers), f32),
            pltpu.VMEM((2, 2, 2, INNER, cy, layers), f32),
            pltpu.VMEM((2, ny, layers), f32),
            pltpu.VMEM((2, ny, layers), f32),
            pltpu.VMEM((2, nx, layers), f32),
            dma((3,)), dma((4,)),
            dma((2,)), dma((2,)), dma((3, 2)), dma((3, 2)), dma((2, 2)), dma((2, 2)),
            dma((2, 2)), dma((2, 2)), dma((2, 2)), dma((2, 2)), dma((2, 2, 2)), dma((2, 2, 2)),
            dma((2,)), dma((2,)), dma((2,)), dma((2,)),
        ],
        compiler_params=pltpu.CompilerParams(collective_id=0, has_side_effects=True, vmem_limit_bytes=60 * 2**20),
    )(load_terms, start_values, reaction_rate)


def solution(mesh):
    spec = P("band", "lane", None)
    return jax.shard_map(
        functools.partial(shards, mesh.shape["lane"], mesh.shape["band"]),
        mesh=mesh,
        in_specs=(spec, spec, spec),
        out_specs=spec,
        check_vma=False,
    )
```

```python
import functools

import jax
import jax.numpy as jnp
from jax import lax
from jax.experimental import pallas as pl
from jax.experimental.pallas import tpu as pltpu
from jax.sharding import PartitionSpec as P

RATIO = 4
BEFORE = 3
AFTER = 2
INNER = 13
MESH = pl.DeviceIdType.MESH

PAD = 8
DEPTH = BEFORE + 1
ITEMS = BEFORE + 3
CPAD = 16


def kernel(lanes, bands, ny, nx, load_hbm, start_hbm, rate_hbm, out_hbm,
           u0, u1, u2, u3, fl, fw, ca, cb, c0, cw, tmp, stage,
           sx, rx, line, held, csx, crx, crc, hsx, hrx, hry,
           in_sem, out_sem, xs, xr, ys, yr, kxs, kxr, kys, kyr, kcs, kcr, hxs, hxr, hys, hyr):
    lane, band = lax.axis_index("lane"), lax.axis_index("band")
    sides = ({"lane": lax.rem(lane + lanes - 1, lanes)}, {"lane": lax.rem(lane + 1, lanes)})
    ends = ({"band": lax.rem(band + bands - 1, bands)}, {"band": lax.rem(band + 1, bands)})
    ry, wx = ny + 2 * DEPTH, nx + 2 * PAD
    cy, cx = ny // RATIO, nx // RATIO
    cwx = cx + 2 * CPAD
    flat = lambda ref: ref.reshape(ref.shape[0] * ref.shape[1], ref.shape[2])
    fu0, fu1, fu2, fu3, ffl, ffw = flat(u0), flat(u1), flat(u2), flat(u3), flat(fl), flat(fw)
    fca, fcb, fc0, fcw = flat(ca), flat(cb), flat(c0), flat(cw)
    own = (pl.ds(DEPTH, ny), pl.ds(PAD, nx))

    cols = (pl.ds(PAD, 8), pl.ds(PAD + nx - 8, 8), pl.ds(PAD + 8, nx - 16))
    takes = (pl.ds(0, 8), pl.ds(nx - 8, 8), pl.ds(8, nx - 16))
    ins = []
    for part in range(3):
        for n, (src, dst) in enumerate(((start_hbm, u0), (load_hbm, fl), (rate_hbm, fw))):
            copy = pltpu.make_async_copy(src.at[:, takes[part]], dst.at[own[0], cols[part]], in_sem.at[n, part])
            copy.start()
            ins.append(copy)

    barrier = pltpu.get_barrier_semaphore()
    for other in sides + ends:
        pl.semaphore_signal(barrier, inc=1, device_id=other, device_id_type=MESH)
    pl.semaphore_wait(barrier, 4)

    def remote(src, dst, send, recv, other):
        copy = pltpu.make_async_remote_copy(src_ref=src, dst_ref=dst, send_sem=send, recv_sem=recv, device_id=other, device_id_type=MESH)
        copy.start()
        return copy

    def send_edges(part):
        copies = []
        for n, (ref, deep) in enumerate(((u0, DEPTH), (fl, DEPTH - 1), (fw, DEPTH - 1))):
            copies.append(remote(ref.at[pl.ds(DEPTH, deep), cols[part]], ref.at[pl.ds(DEPTH + ny, deep), cols[part]], ys.at[n, part, 0], yr.at[n, part, 1], ends[0]))
            copies.append(remote(ref.at[pl.ds(DEPTH + ny - deep, deep), cols[part]], ref.at[pl.ds(DEPTH - deep, deep), cols[part]], ys.at[n, part, 1], yr.at[n, part, 0], ends[1]))
        return copies

    for copy in ins[:6]:
        copy.wait()
    edge_copies = send_edges(0) + send_edges(1)

    def column(ref, col, first=0, count=ry):
        return ref[pl.ds(first * wx + col, count, stride=wx), :]

    for ref in (fu0, fu1, fu2):
        for col in (PAD - 1, PAD + nx):
            ref[pl.ds(col, ry, stride=wx), :] = jnp.zeros((ry, ref.shape[1]), jnp.float32)
    for copy in edge_copies:
        copy.wait()

    inner = pl.ds(8, ry)

    def about(ref):
        return ref[pl.ds(7, ry), :] + ref[pl.ds(9, ry), :]

    x_copies = []
    kept = []
    for side in range(2):
        where = [PAD + d if side == 0 else PAD + nx - 1 - d for d in range(DEPTH)]
        values = [column(fu0, col) for col in where]
        weights = [0.8 / (4.0 + column(ffw, col)) for col in where[:3]]
        loads = [weight * column(ffl, col) for weight, col in zip(weights, where)]
        sx[side, 0] = values[0]
        sx[side, 1] = weights[0]
        sx[side, 2] = weights[0] * weights[0] * weights[1]
        sx[side, 3] = weights[0] * values[1] + loads[0]
        x_copies.append(remote(sx.at[side, pl.ds(0, 4)], rx.at[1 - side, pl.ds(0, 4)], xs.at[side, 0], xr.at[1 - side, 0], sides[side]))
        for d in range(3):
            line[d, inner] = values[d]
        once = []
        for d in range(3):
            around = about(line.at[d]) + values[d + 1]
            if d > 0:
                around = around + values[d - 1]
            once.append(0.2 * values[d] + weights[d] * around + loads[d])
        sx[side, 4] = weights[0] * once[1] + loads[0]
        line[3, inner] = once[1]
        twice = 0.2 * once[1] + weights[1] * (about(line.at[3]) + once[0] + once[2]) + loads[1]
        sx[side, 5] = weights[0] * twice + loads[0]
        x_copies.append(remote(sx.at[side, pl.ds(4, 2)], rx.at[1 - side, pl.ds(4, 2)], xs.at[side, 1], xr.at[1 - side, 1], sides[side]))

    for copy in ins[6:]:
        copy.wait()
    mid_copies = send_edges(2)

    def blocks(rows_of, n):
        total = rows_of(0)
        for r in range(1, RATIO):
            total = total + rows_of(r)
        tmp[pl.ds(pl.multiple_of(n * wx, 8), nx), :] = total

    def across(n):
        base = n * wx
        total = tmp[pl.ds(base, cx, stride=RATIO), :]
        for j in range(1, RATIO):
            total = total + tmp[pl.ds(base + j, cx, stride=RATIO), :]
        return total * (1.0 / RATIO)

    def coarse_at(n):
        return pl.ds(pl.multiple_of((CPAD + n) * cwx + CPAD, 8), cx)

    def mass_row(n, carry):
        blocks(lambda r: ffw[pl.ds(pl.multiple_of((DEPTH + n * RATIO + r) * wx + PAD, 8), nx), :], n)
        fcw[coarse_at(n), :] = 0.8 / (4.0 + across(n))
        return carry

    lax.fori_loop(0, cy, mass_row, 0)

    def send_coarse(q, src):
        copies = []
        for side in range(2):
            for d in range(INNER):
                col = d if side == 0 else cx - 1 - d
                csx[side, q, d] = src[pl.ds(CPAD * cwx + CPAD + col, cy, stride=cwx), :]
            copies.append(remote(csx.at[side, q], crx.at[1 - side, q], kxs.at[side, q], kxr.at[1 - side, q], sides[side]))
        return copies

    def send_rows(q, ref):
        mine = ref.at[pl.ds(CPAD, cy), pl.ds(CPAD, cx)]
        return [
            remote(mine, ref.at[pl.ds(CPAD + cy, cy), pl.ds(CPAD, cx)], kys.at[0, q], kyr.at[1, q], ends[0]),
            remote(mine, ref.at[pl.ds(CPAD - cy, cy), pl.ds(CPAD, cx)], kys.at[1, q], kyr.at[0, q], ends[1]),
        ]

    def forward(q, side):
        return [remote(crx.at[side, q], crc.at[side, q, 1 - end], kcs.at[side, q, end], kcr.at[side, q, 1 - end], ends[end]) for end in range(2)]

    def unpack_coarse(q, dst):
        for side in range(2):
            for d in range(INNER):
                col = CPAD - 1 - d if side == 0 else CPAD + cx + d
                dst[pl.ds(CPAD * cwx + col, cy, stride=cwx), :] = crx[side, q, d]
                dst[pl.ds((CPAD - cy) * cwx + col, cy, stride=cwx), :] = crc[side, q, 0, d]
                dst[pl.ds((CPAD + cy) * cwx + col, cy, stride=cwx), :] = crc[side, q, 1, d]

    mass_x = send_coarse(0, fcw)
    mass_y = send_rows(0, cw)

    for copy in mid_copies:
        copy.wait()

    def weigh(y, carry):
        at = pl.ds(pl.multiple_of(y * wx + PAD, 8), nx)
        weight = 0.8 / (4.0 + ffw[at, :])
        ffw[at, :] = weight
        ffl[at, :] = weight * ffl[at, :]
        return carry

    lax.fori_loop(0, ry, weigh, 0)

    def sweep(src, dst, load, weight, width, first, count, ranges, put=None, group=2):
        def rows(n, carry):
            for r in range(group):
                for low, high in ranges:
                    y = first + group * n + r
                    base = pl.multiple_of(y * width + low, 8)
                    span = high - low
                    here = src[pl.ds(base, span), :]
                    around = (src[pl.ds(base - width, span), :] + src[pl.ds(base + width, span), :]
                              + src[pl.ds(base - 1, span), :] + src[pl.ds(base + 1, span), :])
                    new = 0.2 * here + weight[pl.ds(base, span), :] * around + load[pl.ds(base, span), :]
                    if put is None:
                        dst[pl.ds(base, span), :] = new
                    else:
                        put(y, new)
            return carry

        lax.fori_loop(0, count // group, rows, 0)

    def defect_rows(low, span):
        def row(n, carry):
            total = None
            for r in range(RATIO):
                base = pl.multiple_of((DEPTH + n * RATIO + r) * wx + low, 8)
                around = (fu3[pl.ds(base - wx, span), :] + fu3[pl.ds(base + wx, span), :]
                          + fu3[pl.ds(base - 1, span), :] + fu3[pl.ds(base + 1, span), :])
                here = around + (ffl[pl.ds(base, span), :] - 0.8 * fu3[pl.ds(base, span), :]) / ffw[pl.ds(base, span), :]
                total = here if total is None else total + here
            tmp[pl.ds(pl.multiple_of(n * wx + low - PAD, 8), span), :] = total
            return carry

        lax.fori_loop(0, cy, row, 0)

    whole = ((PAD, PAD + nx),)
    sweep(fu0, fu1, ffl, ffw, wx, 1, ry - 2, whole)
    sweep(fu1, fu2, ffl, ffw, wx, 2, ry - 4, whole)
    sweep(fu2, fu3, ffl, ffw, wx, 3, ry - 6, whole)
    defect_rows(PAD + 8, nx - 16)

    for copy in x_copies:
        copy.wait_recv()
    edges = ((PAD, PAD + 8), (PAD + nx - 8, PAD + nx))
    lanes_of = ((PAD - 1, PAD), (PAD + nx, PAD + nx - 1))
    fine = (fu0, fu1, fu2, fu3)
    for t in range(BEFORE):
        for side, (halo, near) in enumerate(lanes_of):
            if t == 0:
                held[side, 0, inner] = rx[side, 0]
            here = held[side, t, inner]
            fine[t][pl.ds(halo, ry, stride=wx), :] = here
            new = 0.2 * here + rx[side, 1] * (about(held.at[side, t]) + column(fine[t], near)) + rx[side, 3 + t]
            if t == 2:
                new = new + rx[side, 2] * column(fu0, near)
            held[side, t + 1, inner] = new
        sweep(fine[t], fine[t + 1], ffl, ffw, wx, 1, ry - 2, edges, None, 10 if (ry - 2) % 10 == 0 else 2)
    for side, (halo, near) in enumerate(lanes_of):
        fu3[pl.ds(halo, ry, stride=wx), :] = held[side, BEFORE, inner]
    for low, high in edges:
        defect_rows(low, high - low)

    h_copies = []

    def load_row(n, carry):
        fc0[coarse_at(n), :] = fcw[coarse_at(n), :] * across(n)
        return carry

    lax.fori_loop(0, cy, load_row, 0)

    load_x = send_coarse(1, fc0)
    load_y = send_rows(1, c0)
    for side in range(2):
        col, second = (PAD, PAD + 1) if side == 0 else (PAD + nx - 1, PAD + nx - 2)
        hsx[side] = column(ffw, col, DEPTH, ny) * column(fu3, second, DEPTH, ny) + column(ffl, col, DEPTH, ny)
        h_copies.append(remote(hsx.at[side], hrx.at[1 - side], hxs.at[side], hxr.at[1 - side], sides[side]))
    hy_copies = [
        remote(u3.at[DEPTH + 1, own[1]], hry.at[1], hys.at[0], hyr.at[1], ends[0]),
        remote(u3.at[DEPTH + ny - 2, own[1]], hry.at[0], hys.at[1], hyr.at[0], ends[1]),
    ]
    forwards = []
    for side in range(2):
        mass_x[1 - side].wait_recv()
        forwards += forward(0, side)
    for copy in mass_y + forwards:
        copy.wait()
    unpack_coarse(0, fcw)
    forwards = []
    for side in range(2):
        load_x[1 - side].wait_recv()
        forwards += forward(1, side)
    for copy in load_y + forwards:
        copy.wait()
    unpack_coarse(1, fc0)

    now, later = fc0, fca
    for t in range(2, INNER + 1):
        reach = INNER + 1 - t
        low = (CPAD - reach) // 8 * 8
        high = -((-(CPAD + cx + reach)) // 8) * 8
        sweep(now, later, fc0, fcw, cwx, CPAD - reach, cy + 2 * reach, ((low, high),))
        now, later = later, (fcb if t % 2 == 0 else fca)

    for copy in h_copies:
        copy.wait_recv()
    for copy in hy_copies:
        copy.wait()
    u3[DEPTH - 2, own[1]] = hry[0]
    u3[DEPTH + ny + 1, own[1]] = hry[1]
    count = wx // RATIO
    for n in range(cy + 2):
        row = now[pl.ds((CPAD - 1 + n) * cwx + CPAD - PAD // RATIO, count), :]
        for j in range(RATIO):
            tmp[pl.ds(n * wx + j, count, stride=RATIO), :] = row

    def correct(n, carry):
        extra = tmp[pl.ds(pl.multiple_of(n * wx, 8), wx), :]
        for r in range(RATIO):
            at = pl.ds(pl.multiple_of((n * RATIO + r) * wx, 8), wx)
            fu3[at, :] = fu3[at, :] + extra
        return carry

    lax.fori_loop(0, cy + 2, correct, 0)
    sweep(fu3, fu0, ffl, ffw, wx, DEPTH - 1, ny + 2, whole)
    for side, (halo, near) in enumerate(lanes_of):
        here = column(fu3, halo, DEPTH, ny)
        change = here - held[side, BEFORE, pl.ds(8 + DEPTH, ny)]
        around = column(fu3, halo, DEPTH - 1, ny) + column(fu3, halo, DEPTH + 1, ny) + column(fu3, near, DEPTH, ny) + change
        fu0[pl.ds(DEPTH * wx + halo, ny, stride=wx), :] = 0.2 * here + rx[side, 1, pl.ds(DEPTH, ny)] * around + hrx[side]

    def put(y, new):
        stage[y - DEPTH] = new

    pieces = 4
    outs = []
    for piece in range(pieces):
        part = ny // pieces
        sweep(fu0, None, ffl, ffw, wx, DEPTH + piece * part, part, whole, put)
        at = pl.ds(piece * part, part)
        copy = pltpu.make_async_copy(stage.at[at], out_hbm.at[at], out_sem.at[piece])
        copy.start()
        outs.append(copy)
    for copy in x_copies + mass_x + load_x + h_copies:
        copy.wait_send()
    for copy in outs:
        copy.wait()


def shards(lanes, bands, load_terms, start_values, reaction_rate):
    ny, nx, layers = load_terms.shape
    f32 = jnp.float32
    ry, wx = ny + 2 * DEPTH, nx + 2 * PAD
    cy, cx = ny // RATIO, nx // RATIO
    assert ny % 8 == 0 and nx % 8 == 0 and INNER <= min(cy, cx) <= CPAD and layers == 128
    fine = pltpu.VMEM((ry, wx, layers), f32)
    coarse = pltpu.VMEM((cy + 2 * CPAD, cx + 2 * CPAD, layers), f32)
    dma = pltpu.SemaphoreType.DMA
    return pl.pallas_call(
        functools.partial(kernel, lanes, bands, ny, nx),
        out_shape=jax.ShapeDtypeStruct(load_terms.shape, f32),
        in_specs=[pl.BlockSpec(memory_space=pl.ANY)] * 3,
        out_specs=pl.BlockSpec(memory_space=pl.ANY),
        scratch_shapes=[
            fine, fine, fine, fine, fine, fine, coarse, coarse, coarse, coarse,
            pltpu.VMEM(((cy + 2) * wx, layers), f32),
            pltpu.VMEM((ny, nx, layers), f32),
            pltpu.VMEM((2, ITEMS, ry, layers), f32),
            pltpu.VMEM((2, ITEMS, ry, layers), f32),
            pltpu.VMEM((4, ry + 16, layers), f32),
            pltpu.VMEM((2, DEPTH, ry + 16, layers), f32),
            pltpu.VMEM((2, 2, INNER, cy, layers), f32),
            pltpu.VMEM((2, 2, INNER, cy, layers), f32),
            pltpu.VMEM((2, 2, 2, INNER, cy, layers), f32),
            pltpu.VMEM((2, ny, layers), f32),
            pltpu.VMEM((2, ny, layers), f32),
            pltpu.VMEM((2, nx, layers), f32),
            dma((3, 3)), dma((4,)),
            dma((2, 2)), dma((2, 2)), dma((3, 3, 2)), dma((3, 3, 2)),
            dma((2, 2)), dma((2, 2)), dma((2, 2)), dma((2, 2)), dma((2, 2, 2)), dma((2, 2, 2)),
            dma((2,)), dma((2,)), dma((2,)), dma((2,)),
        ],
        compiler_params=pltpu.CompilerParams(collective_id=0, has_side_effects=True, vmem_limit_bytes=60 * 2**20),
    )(load_terms, start_values, reaction_rate)


def solution(mesh):
    spec = P("band", "lane", None)
    return jax.shard_map(
        functools.partial(shards, mesh.shape["lane"], mesh.shape["band"]),
        mesh=mesh,
        in_specs=(spec, spec, spec),
        out_specs=spec,
        check_vma=False,
    )
```

```python
import functools

import jax
import jax.numpy as jnp
from jax import lax
from jax.experimental import pallas as pl
from jax.experimental.pallas import tpu as pltpu
from jax.sharding import PartitionSpec as P

RATIO = 4
BEFORE = 3
AFTER = 2
INNER = 13
MESH = pl.DeviceIdType.MESH

PAD = 8
DEPTH = BEFORE + 1
ITEMS = BEFORE + 3
CPAD = 16


def kernel(lanes, bands, ny, nx, load_hbm, start_hbm, rate_hbm, out_hbm,
           u0, u1, u2, u3, fl, fw, ca, cb, c0, cw, tmp, stage,
           sx, rx, line, held, csx, crx, crc, hsx, hrx, hry,
           in_sem, out_sem, xs, xr, ys, yr, kxs, kxr, kys, kyr, kcs, kcr, hxs, hxr, hys, hyr):
    lane, band = lax.axis_index("lane"), lax.axis_index("band")
    sides = ({"lane": lax.rem(lane + lanes - 1, lanes)}, {"lane": lax.rem(lane + 1, lanes)})
    ends = ({"band": lax.rem(band + bands - 1, bands)}, {"band": lax.rem(band + 1, bands)})
    ry, wx = ny + 2 * DEPTH, nx + 2 * PAD
    cy, cx = ny // RATIO, nx // RATIO
    cwx = cx + 2 * CPAD
    flat = lambda ref: ref.reshape(ref.shape[0] * ref.shape[1], ref.shape[2])
    fu0, fu1, fu2, fu3, ffl, ffw = flat(u0), flat(u1), flat(u2), flat(u3), flat(fl), flat(fw)
    fca, fcb, fc0, fcw = flat(ca), flat(cb), flat(c0), flat(cw)
    own = (pl.ds(DEPTH, ny), pl.ds(PAD, nx))

    cols = (pl.ds(PAD, 8), pl.ds(PAD + nx - 8, 8), pl.ds(PAD + 8, nx - 16))
    takes = (pl.ds(0, 8), pl.ds(nx - 8, 8), pl.ds(8, nx - 16))
    ins = []
    for part in range(3):
        for n, (src, dst) in enumerate(((start_hbm, u0), (load_hbm, fl), (rate_hbm, fw))):
            copy = pltpu.make_async_copy(src.at[:, takes[part]], dst.at[own[0], cols[part]], in_sem.at[n, part])
            copy.start()
            ins.append(copy)

    barrier = pltpu.get_barrier_semaphore()
    for other in sides + ends:
        pl.semaphore_signal(barrier, inc=1, device_id=other, device_id_type=MESH)
    pl.semaphore_wait(barrier, 4)

    def remote(src, dst, send, recv, other):
        copy = pltpu.make_async_remote_copy(src_ref=src, dst_ref=dst, send_sem=send, recv_sem=recv, device_id=other, device_id_type=MESH)
        copy.start()
        return copy

    def send_edges(part):
        copies = []
        for n, (ref, deep) in enumerate(((u0, DEPTH), (fl, DEPTH - 1), (fw, DEPTH - 1))):
            copies.append(remote(ref.at[pl.ds(DEPTH, deep), cols[part]], ref.at[pl.ds(DEPTH + ny, deep), cols[part]], ys.at[n, part, 0], yr.at[n, part, 1], ends[0]))
            copies.append(remote(ref.at[pl.ds(DEPTH + ny - deep, deep), cols[part]], ref.at[pl.ds(DEPTH - deep, deep), cols[part]], ys.at[n, part, 1], yr.at[n, part, 0], ends[1]))
        return copies

    for copy in ins[:6]:
        copy.wait()
    edge_copies = send_edges(0) + send_edges(1)

    def column(ref, col, first=0, count=ry):
        return ref[pl.ds(first * wx + col, count, stride=wx), :]

    for ref in (fu0, fu1, fu2):
        for col in (PAD - 1, PAD + nx):
            ref[pl.ds(col, ry, stride=wx), :] = jnp.zeros((ry, ref.shape[1]), jnp.float32)
    for copy in edge_copies:
        copy.wait()

    inner = pl.ds(8, ry)

    def about(ref):
        return ref[pl.ds(7, ry), :] + ref[pl.ds(9, ry), :]

    x_copies = []
    kept = []
    for side in range(2):
        where = [PAD + d if side == 0 else PAD + nx - 1 - d for d in range(DEPTH)]
        values = [column(fu0, col) for col in where]
        weights = [0.8 / (4.0 + column(ffw, col)) for col in where[:3]]
        loads = [weight * column(ffl, col) for weight, col in zip(weights, where)]
        sx[side, 0] = values[0]
        sx[side, 1] = weights[0]
        sx[side, 2] = weights[0] * weights[0] * weights[1]
        sx[side, 3] = weights[0] * values[1] + loads[0]
        x_copies.append(remote(sx.at[side, pl.ds(0, 4)], rx.at[1 - side, pl.ds(0, 4)], xs.at[side, 0], xr.at[1 - side, 0], sides[side]))
        for d in range(3):
            line[d, inner] = values[d]
        once = []
        for d in range(3):
            around = about(line.at[d]) + values[d + 1]
            if d > 0:
                around = around + values[d - 1]
            once.append(0.2 * values[d] + weights[d] * around + loads[d])
        sx[side, 4] = weights[0] * once[1] + loads[0]
        line[3, inner] = once[1]
        twice = 0.2 * once[1] + weights[1] * (about(line.at[3]) + once[0] + once[2]) + loads[1]
        sx[side, 5] = weights[0] * twice + loads[0]
        x_copies.append(remote(sx.at[side, pl.ds(4, 2)], rx.at[1 - side, pl.ds(4, 2)], xs.at[side, 1], xr.at[1 - side, 1], sides[side]))

    for copy in ins[6:]:
        copy.wait()
    mid_copies = send_edges(2)

    def blocks(rows_of, n):
        total = rows_of(0)
        for r in range(1, RATIO):
            total = total + rows_of(r)
        tmp[pl.ds(pl.multiple_of(n * wx, 8), nx), :] = total

    def across(n):
        base = n * wx
        total = tmp[pl.ds(base, cx, stride=RATIO), :]
        for j in range(1, RATIO):
            total = total + tmp[pl.ds(base + j, cx, stride=RATIO), :]
        return total * (1.0 / RATIO)

    def coarse_at(n):
        return pl.ds(pl.multiple_of((CPAD + n) * cwx + CPAD, 8), cx)

    def mass_row(n, carry):
        blocks(lambda r: ffw[pl.ds(pl.multiple_of((DEPTH + n * RATIO + r) * wx + PAD, 8), nx), :], n)
        fcw[coarse_at(n), :] = 0.8 / (4.0 + across(n))
        return carry

    lax.fori_loop(0, cy, mass_row, 0)

    def send_coarse(q, src):
        copies = []
        for side in range(2):
            for d in range(INNER):
                col = d if side == 0 else cx - 1 - d
                csx[side, q, d] = src[pl.ds(CPAD * cwx + CPAD + col, cy, stride=cwx), :]
            copies.append(remote(csx.at[side, q], crx.at[1 - side, q], kxs.at[side, q], kxr.at[1 - side, q], sides[side]))
        return copies

    def send_rows(q, ref):
        mine = ref.at[pl.ds(CPAD, cy), pl.ds(CPAD, cx)]
        return [
            remote(mine, ref.at[pl.ds(CPAD + cy, cy), pl.ds(CPAD, cx)], kys.at[0, q], kyr.at[1, q], ends[0]),
            remote(mine, ref.at[pl.ds(CPAD - cy, cy), pl.ds(CPAD, cx)], kys.at[1, q], kyr.at[0, q], ends[1]),
        ]

    def forward(q, side):
        return [remote(crx.at[side, q], crc.at[side, q, 1 - end], kcs.at[side, q, end], kcr.at[side, q, 1 - end], ends[end]) for end in range(2)]

    def unpack_coarse(q, dst):
        for side in range(2):
            for d in range(INNER):
                col = CPAD - 1 - d if side == 0 else CPAD + cx + d
                dst[pl.ds(CPAD * cwx + col, cy, stride=cwx), :] = crx[side, q, d]
                dst[pl.ds((CPAD - cy) * cwx + col, cy, stride=cwx), :] = crc[side, q, 0, d]
                dst[pl.ds((CPAD + cy) * cwx + col, cy, stride=cwx), :] = crc[side, q, 1, d]

    mass_x = send_coarse(0, fcw)
    mass_y = send_rows(0, cw)

    for copy in mid_copies:
        copy.wait()

    def weigh(y, carry):
        at = pl.ds(pl.multiple_of(y * wx + PAD, 8), nx)
        weight = 0.8 / (4.0 + ffw[at, :])
        ffw[at, :] = weight
        ffl[at, :] = weight * ffl[at, :]
        return carry

    lax.fori_loop(0, ry, weigh, 0)

    def sweep(src, dst, load, weight, width, first, count, ranges, put=None, group=2):
        def rows(n, carry):
            for low, high in ranges:
                span = high - low
                base = pl.multiple_of((first + group * n) * width + low, 8)
                above, here = src[pl.ds(base - width, span), :], src[pl.ds(base, span), :]
                for r in range(group):
                    at = base + r * width
                    below = src[pl.ds(at + width, span), :]
                    around = (above + below) + (src[pl.ds(at - 1, span), :] + src[pl.ds(at + 1, span), :])
                    new = 0.2 * here + weight[pl.ds(at, span), :] * around + load[pl.ds(at, span), :]
                    if put is None:
                        dst[pl.ds(at, span), :] = new
                    else:
                        put(first + group * n + r, new)
                    above, here = here, below
            return carry

        lax.fori_loop(0, -(-count // group), rows, 0)

    def defect_rows(ranges):
        def row(n, carry):
            for low, high in ranges:
                span = high - low
                base = pl.multiple_of((DEPTH + n * RATIO) * wx + low, 8)
                above, here = fu3[pl.ds(base - wx, span), :], fu3[pl.ds(base, span), :]
                total = None
                for r in range(RATIO):
                    at = base + r * wx
                    below = fu3[pl.ds(at + wx, span), :]
                    around = (above + below) + (fu3[pl.ds(at - 1, span), :] + fu3[pl.ds(at + 1, span), :])
                    part = around + (ffl[pl.ds(at, span), :] - 0.8 * here) / ffw[pl.ds(at, span), :]
                    total = part if total is None else total + part
                    above, here = here, below
                tmp[pl.ds(pl.multiple_of(n * wx + low - PAD, 8), span), :] = total
            return carry

        lax.fori_loop(0, cy, row, 0)

    whole = ((PAD, PAD + nx),)
    sweep(fu0, fu1, ffl, ffw, wx, 1, ry - 2, whole, None, 7)
    sweep(fu1, fu2, ffl, ffw, wx, 1, ry - 2, whole, None, 7)
    sweep(fu2, fu3, ffl, ffw, wx, 1, ry - 2, whole, None, 7)
    defect_rows(((PAD + 8, PAD + nx - 8),))

    for copy in x_copies:
        copy.wait_recv()
    edges = ((PAD, PAD + 8), (PAD + nx - 8, PAD + nx))
    lanes_of = ((PAD - 1, PAD), (PAD + nx, PAD + nx - 1))
    fine = (fu0, fu1, fu2, fu3)
    for t in range(BEFORE):
        for side, (halo, near) in enumerate(lanes_of):
            if t == 0:
                held[side, 0, inner] = rx[side, 0]
            here = held[side, t, inner]
            fine[t][pl.ds(halo, ry, stride=wx), :] = here
            new = 0.2 * here + rx[side, 1] * (about(held.at[side, t]) + column(fine[t], near)) + rx[side, 3 + t]
            if t == 2:
                new = new + rx[side, 2] * column(fu0, near)
            held[side, t + 1, inner] = new
        sweep(fine[t], fine[t + 1], ffl, ffw, wx, 1, ry - 2, edges, None, 14)
    for side, (halo, near) in enumerate(lanes_of):
        fu3[pl.ds(halo, ry, stride=wx), :] = held[side, BEFORE, inner]
    defect_rows(edges)

    h_copies = []

    def load_row(n, carry):
        fc0[coarse_at(n), :] = fcw[coarse_at(n), :] * across(n)
        return carry

    lax.fori_loop(0, cy, load_row, 0)

    load_x = send_coarse(1, fc0)
    load_y = send_rows(1, c0)
    for side in range(2):
        col, second = (PAD, PAD + 1) if side == 0 else (PAD + nx - 1, PAD + nx - 2)
        hsx[side] = column(ffw, col, DEPTH, ny) * column(fu3, second, DEPTH, ny) + column(ffl, col, DEPTH, ny)
        h_copies.append(remote(hsx.at[side], hrx.at[1 - side], hxs.at[side], hxr.at[1 - side], sides[side]))
    hy_copies = [
        remote(u3.at[DEPTH + 1, own[1]], hry.at[1], hys.at[0], hyr.at[1], ends[0]),
        remote(u3.at[DEPTH + ny - 2, own[1]], hry.at[0], hys.at[1], hyr.at[0], ends[1]),
    ]
    forwards = []
    for side in range(2):
        mass_x[1 - side].wait_recv()
        forwards += forward(0, side)
    for copy in mass_y + forwards:
        copy.wait()
    unpack_coarse(0, fcw)
    forwards = []
    for side in range(2):
        load_x[1 - side].wait_recv()
        forwards += forward(1, side)
    for copy in load_y + forwards:
        copy.wait()
    unpack_coarse(1, fc0)

    now, later = fc0, fca
    for t in range(2, INNER + 1):
        reach = INNER + 1 - t
        low = (CPAD - reach) // 8 * 8
        high = -((-(CPAD + cx + reach)) // 8) * 8
        sweep(now, later, fc0, fcw, cwx, CPAD - reach, cy + 2 * reach, ((low, high),), None, 8)
        now, later = later, (fcb if t % 2 == 0 else fca)

    for copy in h_copies:
        copy.wait_recv()
    for copy in hy_copies:
        copy.wait()
    u3[DEPTH - 2, own[1]] = hry[0]
    u3[DEPTH + ny + 1, own[1]] = hry[1]
    count = wx // RATIO
    for n in range(cy + 2):
        row = now[pl.ds((CPAD - 1 + n) * cwx + CPAD - PAD // RATIO, count), :]
        for j in range(RATIO):
            tmp[pl.ds(n * wx + j, count, stride=RATIO), :] = row

    def correct(n, carry):
        extra = tmp[pl.ds(pl.multiple_of(n * wx, 8), wx), :]
        for r in range(RATIO):
            at = pl.ds(pl.multiple_of((n * RATIO + r) * wx, 8), wx)
            fu3[at, :] = fu3[at, :] + extra
        return carry

    lax.fori_loop(0, cy + 2, correct, 0)
    sweep(fu3, fu0, ffl, ffw, wx, DEPTH - 1, ny + 2, whole, None, 6)
    for side, (halo, near) in enumerate(lanes_of):
        here = column(fu3, halo, DEPTH, ny)
        change = here - held[side, BEFORE, pl.ds(8 + DEPTH, ny)]
        around = column(fu3, halo, DEPTH - 1, ny) + column(fu3, halo, DEPTH + 1, ny) + column(fu3, near, DEPTH, ny) + change
        fu0[pl.ds(DEPTH * wx + halo, ny, stride=wx), :] = 0.2 * here + rx[side, 1, pl.ds(DEPTH, ny)] * around + hrx[side]

    def put(y, new):
        stage[y - DEPTH] = new

    pieces = 4
    outs = []
    for piece in range(pieces):
        part = ny // pieces
        sweep(fu0, None, ffl, ffw, wx, DEPTH + piece * part, part, whole, put, 8)
        at = pl.ds(piece * part, part)
        copy = pltpu.make_async_copy(stage.at[at], out_hbm.at[at], out_sem.at[piece])
        copy.start()
        outs.append(copy)
    for copy in x_copies + mass_x + load_x + h_copies:
        copy.wait_send()
    for copy in outs:
        copy.wait()


def shards(lanes, bands, load_terms, start_values, reaction_rate):
    ny, nx, layers = load_terms.shape
    f32 = jnp.float32
    ry, wx = ny + 2 * DEPTH, nx + 2 * PAD
    cy, cx = ny // RATIO, nx // RATIO
    assert (ry - 2) % 14 == 0 and (ny + 2) % 6 == 0 and ny % 32 == 0 and nx % 8 == 0 and INNER <= min(cy, cx) <= CPAD and layers == 128
    fine = pltpu.VMEM((ry, wx, layers), f32)
    coarse = pltpu.VMEM((cy + 2 * CPAD, cx + 2 * CPAD, layers), f32)
    dma = pltpu.SemaphoreType.DMA
    return pl.pallas_call(
        functools.partial(kernel, lanes, bands, ny, nx),
        out_shape=jax.ShapeDtypeStruct(load_terms.shape, f32),
        in_specs=[pl.BlockSpec(memory_space=pl.ANY)] * 3,
        out_specs=pl.BlockSpec(memory_space=pl.ANY),
        scratch_shapes=[
            fine, fine, fine, fine, fine, fine, coarse, coarse, coarse, coarse,
            pltpu.VMEM(((cy + 2) * wx, layers), f32),
            pltpu.VMEM((ny, nx, layers), f32),
            pltpu.VMEM((2, ITEMS, ry, layers), f32),
            pltpu.VMEM((2, ITEMS, ry, layers), f32),
            pltpu.VMEM((4, ry + 16, layers), f32),
            pltpu.VMEM((2, DEPTH, ry + 16, layers), f32),
            pltpu.VMEM((2, 2, INNER, cy, layers), f32),
            pltpu.VMEM((2, 2, INNER, cy, layers), f32),
            pltpu.VMEM((2, 2, 2, INNER, cy, layers), f32),
            pltpu.VMEM((2, ny, layers), f32),
            pltpu.VMEM((2, ny, layers), f32),
            pltpu.VMEM((2, nx, layers), f32),
            dma((3, 3)), dma((4,)),
            dma((2, 2)), dma((2, 2)), dma((3, 3, 2)), dma((3, 3, 2)),
            dma((2, 2)), dma((2, 2)), dma((2, 2)), dma((2, 2)), dma((2, 2, 2)), dma((2, 2, 2)),
            dma((2,)), dma((2,)), dma((2,)), dma((2,)),
        ],
        compiler_params=pltpu.CompilerParams(collective_id=0, has_side_effects=True, vmem_limit_bytes=60 * 2**20),
    )(load_terms, start_values, reaction_rate)


def solution(mesh):
    spec = P("band", "lane", None)
    return jax.shard_map(
        functools.partial(shards, mesh.shape["lane"], mesh.shape["band"]),
        mesh=mesh,
        in_specs=(spec, spec, spec),
        out_specs=spec,
        check_vma=False,
    )
```

```python
import functools

import jax
import jax.numpy as jnp
from jax import lax
from jax.experimental import pallas as pl
from jax.experimental.pallas import tpu as pltpu
from jax.sharding import PartitionSpec as P

RATIO = 4
BEFORE = 3
AFTER = 2
INNER = 13
MESH = pl.DeviceIdType.MESH

PAD = 8
DEPTH = BEFORE + 1
ITEMS = BEFORE + 3
CPAD = 16


def kernel(lanes, bands, ny, nx, load_hbm, start_hbm, rate_hbm, out_hbm,
           u0, u1, u2, u3, fl, fw, ca, cb, c0, cw, tmp, stage,
           sx, rx, line, held, csx, crx, crc, hsx, hrx, hry,
           in_sem, out_sem, xs, xr, ys, yr, kxs, kxr, kys, kyr, kcs, kcr, ws, wr, hxs, hxr, hys, hyr):
    lane, band = lax.axis_index("lane"), lax.axis_index("band")
    sides = ({"lane": lax.rem(lane + lanes - 1, lanes)}, {"lane": lax.rem(lane + 1, lanes)})
    ends = ({"band": lax.rem(band + bands - 1, bands)}, {"band": lax.rem(band + 1, bands)})
    ry, wx = ny + 2 * DEPTH, nx + 2 * PAD
    cy, cx = ny // RATIO, nx // RATIO
    cwx = cx + 2 * CPAD
    flat = lambda ref: ref.reshape(ref.shape[0] * ref.shape[1], ref.shape[2])
    fu0, fu1, fu2, fu3, ffl, ffw = flat(u0), flat(u1), flat(u2), flat(u3), flat(fl), flat(fw)
    fca, fcb, fc0, fcw = flat(ca), flat(cb), flat(c0), flat(cw)
    own = (pl.ds(DEPTH, ny), pl.ds(PAD, nx))

    cols = (pl.ds(PAD, 8), pl.ds(PAD + nx - 8, 8), pl.ds(PAD + 8, nx - 16))
    takes = (pl.ds(0, 8), pl.ds(nx - 8, 8), pl.ds(8, nx - 16))
    ins = []
    for part in range(3):
        for n, (src, dst) in enumerate(((start_hbm, u0), (load_hbm, fl), (rate_hbm, fw))):
            copy = pltpu.make_async_copy(src.at[:, takes[part]], dst.at[own[0], cols[part]], in_sem.at[n, part])
            copy.start()
            ins.append(copy)

    barrier = pltpu.get_barrier_semaphore()
    for other in sides + ends:
        pl.semaphore_signal(barrier, inc=1, device_id=other, device_id_type=MESH)
    pl.semaphore_wait(barrier, 4)

    def remote(src, dst, send, recv, other):
        copy = pltpu.make_async_remote_copy(src_ref=src, dst_ref=dst, send_sem=send, recv_sem=recv, device_id=other, device_id_type=MESH)
        copy.start()
        return copy

    def send_edges(part):
        copies = []
        for n, (ref, deep) in enumerate(((u0, DEPTH), (fl, DEPTH - 1), (fw, DEPTH - 1))):
            copies.append(remote(ref.at[pl.ds(DEPTH, deep), cols[part]], ref.at[pl.ds(DEPTH + ny, deep), cols[part]], ys.at[n, part, 0], yr.at[n, part, 1], ends[0]))
            copies.append(remote(ref.at[pl.ds(DEPTH + ny - deep, deep), cols[part]], ref.at[pl.ds(DEPTH - deep, deep), cols[part]], ys.at[n, part, 1], yr.at[n, part, 0], ends[1]))
        return copies

    for copy in ins[:6]:
        copy.wait()
    edge_copies = send_edges(0) + send_edges(1)

    def column(ref, col, first=0, count=ry):
        return ref[pl.ds(first * wx + col, count, stride=wx), :]

    x_copies = []
    wheres = [[PAD + d if side == 0 else PAD + nx - 1 - d for d in range(DEPTH)] for side in range(2)]
    for side, where in enumerate(wheres):
        first, second = (0.8 / (4.0 + column(ffw, col, DEPTH, ny)) for col in where[:2])
        sx[side, 0, pl.ds(8, ny)] = column(fu0, where[0], DEPTH, ny)
        sx[side, 1, pl.ds(8, ny)] = first
        sx[side, 2, pl.ds(8, ny)] = first * first * second
        sx[side, 3, pl.ds(8, ny)] = first * column(fu0, where[1], DEPTH, ny) + first * column(ffl, where[0], DEPTH, ny)
        x_copies.append(remote(sx.at[side, pl.ds(0, 4), pl.ds(8, ny)], rx.at[1 - side, pl.ds(0, 4), pl.ds(8, ny)], xs.at[side, 0], xr.at[1 - side, 0], sides[side]))

    for ref in (fu0, fu1, fu2):
        for col in (PAD - 1, PAD + nx):
            ref[pl.ds(col, ry, stride=wx), :] = jnp.zeros((ry, ref.shape[1]), jnp.float32)
    for copy in edge_copies:
        copy.wait()

    inner = pl.ds(8, ry)
    reached = pl.ds(8 - DEPTH, ry)

    def about(ref):
        return ref[pl.ds(7, ry), :] + ref[pl.ds(9, ry), :]

    for side, where in enumerate(wheres):
        values = [column(fu0, col) for col in where]
        weights = [0.8 / (4.0 + column(ffw, col)) for col in where[:3]]
        loads = [weight * column(ffl, col) for weight, col in zip(weights, where)]
        for d in range(3):
            line[d, inner] = values[d]
        once = []
        for d in range(3):
            around = about(line.at[d]) + values[d + 1]
            if d > 0:
                around = around + values[d - 1]
            once.append(0.2 * values[d] + weights[d] * around + loads[d])
        sx[side, 4, reached] = weights[0] * once[1] + loads[0]
        line[3, inner] = once[1]
        twice = 0.2 * once[1] + weights[1] * (about(line.at[3]) + once[0] + once[2]) + loads[1]
        sx[side, 5, reached] = weights[0] * twice + loads[0]
        x_copies.append(remote(sx.at[side, pl.ds(4, 2)], rx.at[1 - side, pl.ds(4, 2)], xs.at[side, 1], xr.at[1 - side, 1], sides[side]))

    for copy in ins[6:]:
        copy.wait()
    mid_copies = send_edges(2)

    def blocks(rows_of, n):
        total = rows_of(0)
        for r in range(1, RATIO):
            total = total + rows_of(r)
        tmp[pl.ds(pl.multiple_of(n * wx, 8), nx), :] = total

    def across(n):
        base = n * wx
        total = tmp[pl.ds(base, cx, stride=RATIO), :]
        for j in range(1, RATIO):
            total = total + tmp[pl.ds(base + j, cx, stride=RATIO), :]
        return total * (1.0 / RATIO)

    def coarse_at(n):
        return pl.ds(pl.multiple_of((CPAD + n) * cwx + CPAD, 8), cx)

    def mass_row(n, carry):
        blocks(lambda r: ffw[pl.ds(pl.multiple_of((DEPTH + n * RATIO + r) * wx + PAD, 8), nx), :], n)
        fcw[coarse_at(n), :] = 0.8 / (4.0 + across(n))
        return carry

    lax.fori_loop(0, cy, mass_row, 0)

    def send_coarse(q, src):
        copies = []
        for side in range(2):
            for d in range(INNER):
                col = d if side == 0 else cx - 1 - d
                csx[side, q, d] = src[pl.ds(CPAD * cwx + CPAD + col, cy, stride=cwx), :]
            copies.append(remote(csx.at[side, q], crx.at[1 - side, q], kxs.at[side, q], kxr.at[1 - side, q], sides[side]))
        return copies

    def send_rows(q, ref):
        mine = ref.at[pl.ds(CPAD, cy), pl.ds(CPAD, cx)]
        return [
            remote(mine, ref.at[pl.ds(CPAD + cy, cy), pl.ds(CPAD, cx)], kys.at[0, q], kyr.at[1, q], ends[0]),
            remote(mine, ref.at[pl.ds(CPAD - cy, cy), pl.ds(CPAD, cx)], kys.at[1, q], kyr.at[0, q], ends[1]),
        ]

    def forward(q, side):
        return [remote(crx.at[side, q], crc.at[side, q, 1 - end], kcs.at[side, q, end], kcr.at[side, q, 1 - end], ends[end]) for end in range(1 if bands == 2 else 2)]

    def unpack_coarse(q, dst):
        for side in range(2):
            for d in range(INNER):
                col = CPAD - 1 - d if side == 0 else CPAD + cx + d
                dst[pl.ds(CPAD * cwx + col, cy, stride=cwx), :] = crx[side, q, d]
                dst[pl.ds((CPAD - cy) * cwx + col, cy, stride=cwx), :] = crc[side, q, 1 if bands == 2 else 0, d]
                dst[pl.ds((CPAD + cy) * cwx + col, cy, stride=cwx), :] = crc[side, q, 1, d]

    mass_x = send_coarse(0, fcw)
    mass_y = send_rows(0, cw)

    for copy in mid_copies:
        copy.wait()

    def weigh(y, carry):
        at = pl.ds(pl.multiple_of(y * wx + PAD, 8), nx)
        weight = 0.8 / (4.0 + ffw[at, :])
        ffw[at, :] = weight
        ffl[at, :] = weight * ffl[at, :]
        return carry

    lax.fori_loop(0, ry, weigh, 0)

    def sweep(src, dst, load, weight, width, first, count, ranges, put=None, group=2):
        def rows(n, carry):
            for low, high in ranges:
                span = high - low
                base = pl.multiple_of((first + group * n) * width + low, 8)
                above, here = src[pl.ds(base - width, span), :], src[pl.ds(base, span), :]
                for r in range(group):
                    at = base + r * width
                    below = src[pl.ds(at + width, span), :]
                    around = (above + below) + (src[pl.ds(at - 1, span), :] + src[pl.ds(at + 1, span), :])
                    new = 0.2 * here + weight[pl.ds(at, span), :] * around + load[pl.ds(at, span), :]
                    if put is None:
                        dst[pl.ds(at, span), :] = new
                    else:
                        put(first + group * n + r, new)
                    above, here = here, below
            return carry

        lax.fori_loop(0, -(-count // group), rows, 0)

    def defect_rows(ranges):
        def row(n, carry):
            for low, high in ranges:
                span = high - low
                base = pl.multiple_of((DEPTH + n * RATIO) * wx + low, 8)
                above, here = fu3[pl.ds(base - wx, span), :], fu3[pl.ds(base, span), :]
                total = None
                for r in range(RATIO):
                    at = base + r * wx
                    below = fu3[pl.ds(at + wx, span), :]
                    around = (above + below) + (fu3[pl.ds(at - 1, span), :] + fu3[pl.ds(at + 1, span), :])
                    part = around + (ffl[pl.ds(at, span), :] - 0.8 * here) / ffw[pl.ds(at, span), :]
                    total = part if total is None else total + part
                    above, here = here, below
                tmp[pl.ds(pl.multiple_of(n * wx + low - PAD, 8), span), :] = total
            return carry

        lax.fori_loop(0, cy, row, 0)

    whole = ((PAD, PAD + nx),)
    sweep(fu0, fu1, ffl, ffw, wx, 1, ry - 2, whole, None, 7)
    sweep(fu1, fu2, ffl, ffw, wx, 1, ry - 2, whole, None, 7)
    sweep(fu2, fu3, ffl, ffw, wx, 1, ry - 2, whole, None, 7)
    defect_rows(((PAD + 8, PAD + nx - 8),))

    corners = []
    for side in range(2):
        x_copies[1 - side].wait_recv()
        for end, (take, give) in enumerate(((8, 8 + ny), (ny, 0))):
            corners.append(remote(rx.at[side, pl.ds(0, 4), pl.ds(take, 8)], rx.at[side, pl.ds(0, 4), pl.ds(give, 8)], ws.at[side, end], wr.at[side, 1 - end], ends[end]))
    for copy in x_copies[2:]:
        copy.wait_recv()
    for copy in corners:
        copy.wait()
    edges = ((PAD, PAD + 8), (PAD + nx - 8, PAD + nx))
    lanes_of = ((PAD - 1, PAD), (PAD + nx, PAD + nx - 1))
    fine = (fu0, fu1, fu2, fu3)
    for t in range(BEFORE):
        for side, (halo, near) in enumerate(lanes_of):
            if t == 0:
                held[side, 0, inner] = rx[side, 0, reached]
            here = held[side, t, inner]
            fine[t][pl.ds(halo, ry, stride=wx), :] = here
            new = 0.2 * here + rx[side, 1, reached] * (about(held.at[side, t]) + column(fine[t], near)) + rx[side, 3 + t, reached]
            if t == 2:
                new = new + rx[side, 2, reached] * column(fu0, near)
            held[side, t + 1, inner] = new
        sweep(fine[t], fine[t + 1], ffl, ffw, wx, 1, ry - 2, edges, None, 14)
    for side, (halo, near) in enumerate(lanes_of):
        fu3[pl.ds(halo, ry, stride=wx), :] = held[side, BEFORE, inner]
    defect_rows(edges)

    h_copies = []

    def load_row(n, carry):
        fc0[coarse_at(n), :] = fcw[coarse_at(n), :] * across(n)
        return carry

    lax.fori_loop(0, cy, load_row, 0)

    load_x = send_coarse(1, fc0)
    load_y = send_rows(1, c0)
    for side in range(2):
        col, second = (PAD, PAD + 1) if side == 0 else (PAD + nx - 1, PAD + nx - 2)
        hsx[side] = column(ffw, col, DEPTH, ny) * column(fu3, second, DEPTH, ny) + column(ffl, col, DEPTH, ny)
        h_copies.append(remote(hsx.at[side], hrx.at[1 - side], hxs.at[side], hxr.at[1 - side], sides[side]))
    hy_copies = [
        remote(u3.at[DEPTH + 1, own[1]], hry.at[1], hys.at[0], hyr.at[1], ends[0]),
        remote(u3.at[DEPTH + ny - 2, own[1]], hry.at[0], hys.at[1], hyr.at[0], ends[1]),
    ]
    forwards = []
    for side in range(2):
        mass_x[1 - side].wait_recv()
        forwards += forward(0, side)
    for copy in mass_y + forwards:
        copy.wait()
    unpack_coarse(0, fcw)
    forwards = []
    for side in range(2):
        load_x[1 - side].wait_recv()
        forwards += forward(1, side)
    for copy in load_y + forwards:
        copy.wait()
    unpack_coarse(1, fc0)

    now, later = fc0, fca
    for t in range(2, INNER + 1):
        reach = INNER + 1 - t
        low = (CPAD - reach) // 8 * 8
        high = -((-(CPAD + cx + reach)) // 8) * 8
        sweep(now, later, fc0, fcw, cwx, CPAD - reach, cy + 2 * reach, ((low, high),), None, 8)
        now, later = later, (fcb if t % 2 == 0 else fca)

    for copy in h_copies:
        copy.wait_recv()
    for copy in hy_copies:
        copy.wait()
    u3[DEPTH - 2, own[1]] = hry[0]
    u3[DEPTH + ny + 1, own[1]] = hry[1]
    count = wx // RATIO
    for n in range(cy + 2):
        row = now[pl.ds((CPAD - 1 + n) * cwx + CPAD - PAD // RATIO, count), :]
        for j in range(RATIO):
            tmp[pl.ds(n * wx + j, count, stride=RATIO), :] = row

    def correct(n, carry):
        extra = tmp[pl.ds(pl.multiple_of(n * wx, 8), wx), :]
        for r in range(RATIO):
            at = pl.ds(pl.multiple_of((n * RATIO + r) * wx, 8), wx)
            fu3[at, :] = fu3[at, :] + extra
        return carry

    lax.fori_loop(0, cy + 2, correct, 0)
    sweep(fu3, fu0, ffl, ffw, wx, DEPTH - 1, ny + 2, whole, None, 6)
    for side, (halo, near) in enumerate(lanes_of):
        here = column(fu3, halo, DEPTH, ny)
        change = here - held[side, BEFORE, pl.ds(8 + DEPTH, ny)]
        around = column(fu3, halo, DEPTH - 1, ny) + column(fu3, halo, DEPTH + 1, ny) + column(fu3, near, DEPTH, ny) + change
        fu0[pl.ds(DEPTH * wx + halo, ny, stride=wx), :] = 0.2 * here + rx[side, 1, pl.ds(8, ny)] * around + hrx[side]

    def put(y, new):
        stage[y - DEPTH] = new

    pieces = ny // 8
    outs = []
    for piece in range(pieces):
        part = ny // pieces
        sweep(fu0, None, ffl, ffw, wx, DEPTH + piece * part, part, whole, put, 8)
        at = pl.ds(piece * part, part)
        copy = pltpu.make_async_copy(stage.at[at], out_hbm.at[at], out_sem.at[piece])
        copy.start()
        outs.append(copy)
    for copy in x_copies + mass_x + load_x + h_copies:
        copy.wait_send()
    for copy in outs:
        copy.wait()


def shards(lanes, bands, load_terms, start_values, reaction_rate):
    ny, nx, layers = load_terms.shape
    f32 = jnp.float32
    ry, wx = ny + 2 * DEPTH, nx + 2 * PAD
    cy, cx = ny // RATIO, nx // RATIO
    assert (ry - 2) % 14 == 0 and (ny + 2) % 6 == 0 and ny % 32 == 0 and nx % 8 == 0 and INNER <= min(cy, cx) <= CPAD and layers == 128
    fine = pltpu.VMEM((ry, wx, layers), f32)
    coarse = pltpu.VMEM((cy + 2 * CPAD, cx + 2 * CPAD, layers), f32)
    dma = pltpu.SemaphoreType.DMA
    return pl.pallas_call(
        functools.partial(kernel, lanes, bands, ny, nx),
        out_shape=jax.ShapeDtypeStruct(load_terms.shape, f32),
        in_specs=[pl.BlockSpec(memory_space=pl.ANY)] * 3,
        out_specs=pl.BlockSpec(memory_space=pl.ANY),
        scratch_shapes=[
            fine, fine, fine, fine, fine, fine, coarse, coarse, coarse, coarse,
            pltpu.VMEM(((cy + 2) * wx, layers), f32),
            pltpu.VMEM((ny, nx, layers), f32),
            pltpu.VMEM((2, ITEMS, ny + 16, layers), f32),
            pltpu.VMEM((2, ITEMS, ny + 16, layers), f32),
            pltpu.VMEM((4, ry + 16, layers), f32),
            pltpu.VMEM((2, DEPTH, ry + 16, layers), f32),
            pltpu.VMEM((2, 2, INNER, cy, layers), f32),
            pltpu.VMEM((2, 2, INNER, cy, layers), f32),
            pltpu.VMEM((2, 2, 2, INNER, cy, layers), f32),
            pltpu.VMEM((2, ny, layers), f32),
            pltpu.VMEM((2, ny, layers), f32),
            pltpu.VMEM((2, nx, layers), f32),
            dma((3, 3)), dma((ny // 8,)),
            dma((2, 2)), dma((2, 2)), dma((3, 3, 2)), dma((3, 3, 2)),
            dma((2, 2)), dma((2, 2)), dma((2, 2)), dma((2, 2)), dma((2, 2, 2)), dma((2, 2, 2)), dma((2, 2)), dma((2, 2)),
            dma((2,)), dma((2,)), dma((2,)), dma((2,)),
        ],
        compiler_params=pltpu.CompilerParams(collective_id=0, has_side_effects=True, vmem_limit_bytes=60 * 2**20),
    )(load_terms, start_values, reaction_rate)


def solution(mesh):
    spec = P("band", "lane", None)
    return jax.shard_map(
        functools.partial(shards, mesh.shape["lane"], mesh.shape["band"]),
        mesh=mesh,
        in_specs=(spec, spec, spec),
        out_specs=spec,
        check_vma=False,
    )
```

```python
import functools

import jax
import jax.numpy as jnp
from jax import lax
from jax.experimental import pallas as pl
from jax.experimental.pallas import tpu as pltpu
from jax.sharding import PartitionSpec as P

RATIO = 4
BEFORE = 3
AFTER = 2
INNER = 13
MESH = pl.DeviceIdType.MESH

PAD = 8
DEPTH = BEFORE + 1
ITEMS = BEFORE + 3
CPAD = 16


def kernel(lanes, bands, ny, nx, load_hbm, start_hbm, rate_hbm, out_hbm,
           u0, u1, u2, u3, fl, fw, ca, cb, c0, cw, tmp, stage,
           sx, rx, line, held, csx, crx, crc, hsx, hrx, hry,
           in_sem, out_sem, xs, xr, ys, yr, kxs, kxr, kys, kyr, kcs, kcr, ws, wr, hxs, hxr, hys, hyr):
    lane, band = lax.axis_index("lane"), lax.axis_index("band")
    sides = ({"lane": lax.rem(lane + lanes - 1, lanes)}, {"lane": lax.rem(lane + 1, lanes)})
    ends = ({"band": lax.rem(band + bands - 1, bands)}, {"band": lax.rem(band + 1, bands)})
    ry, wx = ny + 2 * DEPTH, nx + 2 * PAD
    cy, cx = ny // RATIO, nx // RATIO
    cwx = cx + 2 * CPAD
    flat = lambda ref: ref.reshape(ref.shape[0] * ref.shape[1], ref.shape[2])
    fu0, fu1, fu2, fu3, ffl, ffw = flat(u0), flat(u1), flat(u2), flat(u3), flat(fl), flat(fw)
    fca, fcb, fc0, fcw = flat(ca), flat(cb), flat(c0), flat(cw)
    own = (pl.ds(DEPTH, ny), pl.ds(PAD, nx))

    cols = (pl.ds(PAD, 8), pl.ds(PAD + nx - 8, 8), pl.ds(PAD + 8, nx - 16))
    takes = (pl.ds(0, 8), pl.ds(nx - 8, 8), pl.ds(8, nx - 16))
    ins = []
    for part in range(3):
        for n, (src, dst) in enumerate(((start_hbm, u0), (load_hbm, fl), (rate_hbm, fw))):
            copy = pltpu.make_async_copy(src.at[:, takes[part]], dst.at[own[0], cols[part]], in_sem.at[n, part])
            copy.start()
            ins.append(copy)

    barrier = pltpu.get_barrier_semaphore()
    for other in sides + ends:
        pl.semaphore_signal(barrier, inc=1, device_id=other, device_id_type=MESH)
    pl.semaphore_wait(barrier, 4)

    def remote(src, dst, send, recv, other):
        copy = pltpu.make_async_remote_copy(src_ref=src, dst_ref=dst, send_sem=send, recv_sem=recv, device_id=other, device_id_type=MESH)
        copy.start()
        return copy

    def send_edges(part):
        copies = []
        for n, (ref, deep) in enumerate(((u0, DEPTH), (fl, DEPTH - 1), (fw, DEPTH - 1))):
            copies.append(remote(ref.at[pl.ds(DEPTH, deep), cols[part]], ref.at[pl.ds(DEPTH + ny, deep), cols[part]], ys.at[n, part, 0], yr.at[n, part, 1], ends[0]))
            copies.append(remote(ref.at[pl.ds(DEPTH + ny - deep, deep), cols[part]], ref.at[pl.ds(DEPTH - deep, deep), cols[part]], ys.at[n, part, 1], yr.at[n, part, 0], ends[1]))
        return copies

    for copy in ins[:6]:
        copy.wait()
    edge_copies = send_edges(0) + send_edges(1)

    def column(ref, col, first=0, count=ry):
        return ref[pl.ds(first * wx + col, count, stride=wx), :]

    x_copies = []
    wheres = [[PAD + d if side == 0 else PAD + nx - 1 - d for d in range(DEPTH)] for side in range(2)]
    for side, where in enumerate(wheres):
        first, second = (0.8 / (4.0 + column(ffw, col, DEPTH, ny)) for col in where[:2])
        sx[side, 0, pl.ds(8, ny)] = column(fu0, where[0], DEPTH, ny)
        sx[side, 1, pl.ds(8, ny)] = first
        sx[side, 2, pl.ds(8, ny)] = first * first * second
        sx[side, 3, pl.ds(8, ny)] = first * column(fu0, where[1], DEPTH, ny) + first * column(ffl, where[0], DEPTH, ny)
        x_copies.append(remote(sx.at[side, pl.ds(0, 4), pl.ds(8, ny)], rx.at[1 - side, pl.ds(0, 4), pl.ds(8, ny)], xs.at[side, 0], xr.at[1 - side, 0], sides[side]))

    for ref in (fu0, fu1, fu2):
        for col in (PAD - 1, PAD + nx):
            ref[pl.ds(col, ry, stride=wx), :] = jnp.zeros((ry, ref.shape[1]), jnp.float32)
    for copy in edge_copies:
        copy.wait()

    inner = pl.ds(8, ry)
    reached = pl.ds(8 - DEPTH, ry)

    def about(ref):
        return ref[pl.ds(7, ry), :] + ref[pl.ds(9, ry), :]

    for side, where in enumerate(wheres):
        values = [column(fu0, col) for col in where]
        weights = [0.8 / (4.0 + column(ffw, col)) for col in where[:3]]
        loads = [weight * column(ffl, col) for weight, col in zip(weights, where)]
        for d in range(3):
            line[d, inner] = values[d]
        once = []
        for d in range(3):
            around = about(line.at[d]) + values[d + 1]
            if d > 0:
                around = around + values[d - 1]
            once.append(0.2 * values[d] + weights[d] * around + loads[d])
        sx[side, 4, reached] = weights[0] * once[1] + loads[0]
        line[3, inner] = once[1]
        twice = 0.2 * once[1] + weights[1] * (about(line.at[3]) + once[0] + once[2]) + loads[1]
        sx[side, 5, reached] = weights[0] * twice + loads[0]
        x_copies.append(remote(sx.at[side, pl.ds(4, 2)], rx.at[1 - side, pl.ds(4, 2)], xs.at[side, 1], xr.at[1 - side, 1], sides[side]))

    for copy in ins[6:]:
        copy.wait()
    mid_copies = send_edges(2)

    def blocks(rows_of, n):
        total = rows_of(0)
        for r in range(1, RATIO):
            total = total + rows_of(r)
        tmp[pl.ds(pl.multiple_of(n * wx, 8), nx), :] = total

    def across(n):
        base = n * wx
        total = tmp[pl.ds(base, cx, stride=RATIO), :]
        for j in range(1, RATIO):
            total = total + tmp[pl.ds(base + j, cx, stride=RATIO), :]
        return total * (1.0 / RATIO)

    def coarse_at(n):
        return pl.ds(pl.multiple_of((CPAD + n) * cwx + CPAD, 8), cx)

    def mass_row(n, carry):
        blocks(lambda r: ffw[pl.ds(pl.multiple_of((DEPTH + n * RATIO + r) * wx + PAD, 8), nx), :], n)
        fcw[coarse_at(n), :] = 0.8 / (4.0 + across(n))
        return carry

    lax.fori_loop(0, cy, mass_row, 0)

    parts = ((0, 0, INNER), (1, 2, INNER), (1, 0, 2))

    def send_coarse(part, src):
        q, shallow, deep = parts[part]
        span = pl.ds(shallow, deep - shallow)
        copies = []
        for side in range(2):
            for d in range(shallow, deep):
                col = d if side == 0 else cx - 1 - d
                csx[side, q, d] = src[pl.ds(CPAD * cwx + CPAD + col, cy, stride=cwx), :]
            copies.append(remote(csx.at[side, q, span], crx.at[1 - side, q, span], kxs.at[side, part], kxr.at[1 - side, part], sides[side]))
        return copies

    def send_rows(q, ref):
        mine = ref.at[pl.ds(CPAD, cy), pl.ds(CPAD, cx)]
        return [
            remote(mine, ref.at[pl.ds(CPAD + cy, cy), pl.ds(CPAD, cx)], kys.at[0, q], kyr.at[1, q], ends[0]),
            remote(mine, ref.at[pl.ds(CPAD - cy, cy), pl.ds(CPAD, cx)], kys.at[1, q], kyr.at[0, q], ends[1]),
        ]

    def forward(part, side):
        q, shallow, deep = parts[part]
        span = pl.ds(shallow, deep - shallow)
        return [remote(crx.at[side, q, span], crc.at[side, q, 1 - end, span], kcs.at[side, part, end], kcr.at[side, part, 1 - end], ends[end]) for end in range(1 if bands == 2 else 2)]

    def unpack_coarse(part, dst):
        q, shallow, deep = parts[part]
        for side in range(2):
            for d in range(shallow, deep):
                col = CPAD - 1 - d if side == 0 else CPAD + cx + d
                dst[pl.ds(CPAD * cwx + col, cy, stride=cwx), :] = crx[side, q, d]
                dst[pl.ds((CPAD - cy) * cwx + col, cy, stride=cwx), :] = crc[side, q, 1 if bands == 2 else 0, d]
                dst[pl.ds((CPAD + cy) * cwx + col, cy, stride=cwx), :] = crc[side, q, 1, d]

    def take_coarse(part, copies, dst):
        forwards = []
        for side in range(2):
            copies[1 - side].wait_recv()
            forwards += forward(part, side)
        for copy in forwards:
            copy.wait()
        unpack_coarse(part, dst)

    mass_x = send_coarse(0, fcw)
    mass_y = send_rows(0, cw)

    for copy in mid_copies:
        copy.wait()

    def weigh(y, carry):
        at = pl.ds(pl.multiple_of(y * wx + PAD, 8), nx)
        weight = 0.8 / (4.0 + ffw[at, :])
        ffw[at, :] = weight
        ffl[at, :] = weight * ffl[at, :]
        return carry

    lax.fori_loop(0, ry, weigh, 0)

    def sweep(src, dst, load, weight, width, first, count, ranges, put=None, group=2):
        def rows(n, carry):
            for low, high in ranges:
                span = high - low
                base = pl.multiple_of((first + group * n) * width + low, 8)
                above, here = src[pl.ds(base - width, span), :], src[pl.ds(base, span), :]
                for r in range(group):
                    at = base + r * width
                    below = src[pl.ds(at + width, span), :]
                    around = (above + below) + (src[pl.ds(at - 1, span), :] + src[pl.ds(at + 1, span), :])
                    new = 0.2 * here + weight[pl.ds(at, span), :] * around + load[pl.ds(at, span), :]
                    if put is None:
                        dst[pl.ds(at, span), :] = new
                    else:
                        put(first + group * n + r, new)
                    above, here = here, below
            return carry

        lax.fori_loop(0, -(-count // group), rows, 0)

    def defect_rows(ranges):
        def row(n, carry):
            for low, high in ranges:
                span = high - low
                base = pl.multiple_of((DEPTH + n * RATIO) * wx + low, 8)
                above, here = fu3[pl.ds(base - wx, span), :], fu3[pl.ds(base, span), :]
                total = None
                for r in range(RATIO):
                    at = base + r * wx
                    below = fu3[pl.ds(at + wx, span), :]
                    around = (above + below) + (fu3[pl.ds(at - 1, span), :] + fu3[pl.ds(at + 1, span), :])
                    part = around + (ffl[pl.ds(at, span), :] - 0.8 * here) / ffw[pl.ds(at, span), :]
                    total = part if total is None else total + part
                    above, here = here, below
                tmp[pl.ds(pl.multiple_of(n * wx + low - PAD, 8), span), :] = total
            return carry

        lax.fori_loop(0, cy, row, 0)

    whole = ((PAD, PAD + nx),)
    sweep(fu0, fu1, ffl, ffw, wx, 1, ry - 2, whole, None, 7)
    sweep(fu1, fu2, ffl, ffw, wx, 1, ry - 2, whole, None, 7)
    sweep(fu2, fu3, ffl, ffw, wx, 1, ry - 2, whole, None, 7)
    defect_rows(((PAD + 8, PAD + nx - 8),))

    def load_row(n, carry):
        fc0[coarse_at(n), :] = fcw[coarse_at(n), :] * across(n)
        return carry

    lax.fori_loop(0, cy, load_row, 0)
    far_x = send_coarse(1, fc0)

    corners = []
    for side in range(2):
        x_copies[1 - side].wait_recv()
        for end, (take, give) in enumerate(((8, 8 + ny), (ny, 0))):
            corners.append(remote(rx.at[side, pl.ds(0, 4), pl.ds(take, 8)], rx.at[side, pl.ds(0, 4), pl.ds(give, 8)], ws.at[side, end], wr.at[side, 1 - end], ends[end]))
    for copy in x_copies[2:]:
        copy.wait_recv()
    for copy in corners:
        copy.wait()
    edges = ((PAD, PAD + 8), (PAD + nx - 8, PAD + nx))
    lanes_of = ((PAD - 1, PAD), (PAD + nx, PAD + nx - 1))
    fine = (fu0, fu1, fu2, fu3)
    for t in range(BEFORE):
        for side, (halo, near) in enumerate(lanes_of):
            if t == 0:
                held[side, 0, inner] = rx[side, 0, reached]
            here = held[side, t, inner]
            fine[t][pl.ds(halo, ry, stride=wx), :] = here
            new = 0.2 * here + rx[side, 1, reached] * (about(held.at[side, t]) + column(fine[t], near)) + rx[side, 3 + t, reached]
            if t == 2:
                new = new + rx[side, 2, reached] * column(fu0, near)
            held[side, t + 1, inner] = new
        sweep(fine[t], fine[t + 1], ffl, ffw, wx, 1, ry - 2, edges, None, 14)
    for side, (halo, near) in enumerate(lanes_of):
        fu3[pl.ds(halo, ry, stride=wx), :] = held[side, BEFORE, inner]
    defect_rows(edges)

    h_copies = []

    lax.fori_loop(0, cy, load_row, 0)

    load_x = send_coarse(2, fc0)
    load_y = send_rows(1, c0)
    for side in range(2):
        col, second = (PAD, PAD + 1) if side == 0 else (PAD + nx - 1, PAD + nx - 2)
        hsx[side] = column(ffw, col, DEPTH, ny) * column(fu3, second, DEPTH, ny) + column(ffl, col, DEPTH, ny)
        h_copies.append(remote(hsx.at[side], hrx.at[1 - side], hxs.at[side], hxr.at[1 - side], sides[side]))
    hy_copies = [
        remote(u3.at[DEPTH + 1, own[1]], hry.at[1], hys.at[0], hyr.at[1], ends[0]),
        remote(u3.at[DEPTH + ny - 2, own[1]], hry.at[0], hys.at[1], hyr.at[0], ends[1]),
    ]
    for copy in mass_y:
        copy.wait()
    take_coarse(0, mass_x, fcw)
    take_coarse(1, far_x, fc0)
    for copy in load_y:
        copy.wait()
    take_coarse(2, load_x, fc0)

    now, later = fc0, fca
    for t in range(2, INNER + 1):
        reach = INNER + 1 - t
        low = (CPAD - reach) // 8 * 8
        high = -((-(CPAD + cx + reach)) // 8) * 8
        sweep(now, later, fc0, fcw, cwx, CPAD - reach, cy + 2 * reach, ((low, high),), None, 8)
        now, later = later, (fcb if t % 2 == 0 else fca)

    for copy in h_copies:
        copy.wait_recv()
    for copy in hy_copies:
        copy.wait()
    u3[DEPTH - 2, own[1]] = hry[0]
    u3[DEPTH + ny + 1, own[1]] = hry[1]
    count = wx // RATIO
    for n in range(cy + 2):
        row = now[pl.ds((CPAD - 1 + n) * cwx + CPAD - PAD // RATIO, count), :]
        for j in range(RATIO):
            tmp[pl.ds(n * wx + j, count, stride=RATIO), :] = row

    def correct(n, carry):
        extra = tmp[pl.ds(pl.multiple_of(n * wx, 8), wx), :]
        for r in range(RATIO):
            at = pl.ds(pl.multiple_of((n * RATIO + r) * wx, 8), wx)
            fu3[at, :] = fu3[at, :] + extra
        return carry

    lax.fori_loop(0, cy + 2, correct, 0)
    sweep(fu3, fu0, ffl, ffw, wx, DEPTH - 1, ny + 2, whole, None, 6)
    for side, (halo, near) in enumerate(lanes_of):
        here = column(fu3, halo, DEPTH, ny)
        change = here - held[side, BEFORE, pl.ds(8 + DEPTH, ny)]
        around = column(fu3, halo, DEPTH - 1, ny) + column(fu3, halo, DEPTH + 1, ny) + column(fu3, near, DEPTH, ny) + change
        fu0[pl.ds(DEPTH * wx + halo, ny, stride=wx), :] = 0.2 * here + rx[side, 1, pl.ds(8, ny)] * around + hrx[side]

    def put(y, new):
        stage[y - DEPTH] = new

    pieces = ny // 8
    outs = []
    for piece in range(pieces):
        part = ny // pieces
        sweep(fu0, None, ffl, ffw, wx, DEPTH + piece * part, part, whole, put, 8)
        at = pl.ds(piece * part, part)
        copy = pltpu.make_async_copy(stage.at[at], out_hbm.at[at], out_sem.at[piece])
        copy.start()
        outs.append(copy)
    for copy in x_copies + mass_x + far_x + load_x + h_copies:
        copy.wait_send()
    for copy in outs:
        copy.wait()


def shards(lanes, bands, load_terms, start_values, reaction_rate):
    ny, nx, layers = load_terms.shape
    f32 = jnp.float32
    ry, wx = ny + 2 * DEPTH, nx + 2 * PAD
    cy, cx = ny // RATIO, nx // RATIO
    assert (ry - 2) % 14 == 0 and (ny + 2) % 6 == 0 and ny % 32 == 0 and nx % 8 == 0 and INNER <= min(cy, cx) <= CPAD and layers == 128
    fine = pltpu.VMEM((ry, wx, layers), f32)
    coarse = pltpu.VMEM((cy + 2 * CPAD, cx + 2 * CPAD, layers), f32)
    dma = pltpu.SemaphoreType.DMA
    return pl.pallas_call(
        functools.partial(kernel, lanes, bands, ny, nx),
        out_shape=jax.ShapeDtypeStruct(load_terms.shape, f32),
        in_specs=[pl.BlockSpec(memory_space=pl.ANY)] * 3,
        out_specs=pl.BlockSpec(memory_space=pl.ANY),
        scratch_shapes=[
            fine, fine, fine, fine, fine, fine, coarse, coarse, coarse, coarse,
            pltpu.VMEM(((cy + 2) * wx, layers), f32),
            pltpu.VMEM((ny, nx, layers), f32),
            pltpu.VMEM((2, ITEMS, ny + 16, layers), f32),
            pltpu.VMEM((2, ITEMS, ny + 16, layers), f32),
            pltpu.VMEM((4, ry + 16, layers), f32),
            pltpu.VMEM((2, DEPTH, ry + 16, layers), f32),
            pltpu.VMEM((2, 2, INNER, cy, layers), f32),
            pltpu.VMEM((2, 2, INNER, cy, layers), f32),
            pltpu.VMEM((2, 2, 2, INNER, cy, layers), f32),
            pltpu.VMEM((2, ny, layers), f32),
            pltpu.VMEM((2, ny, layers), f32),
            pltpu.VMEM((2, nx, layers), f32),
            dma((3, 3)), dma((ny // 8,)),
            dma((2, 2)), dma((2, 2)), dma((3, 3, 2)), dma((3, 3, 2)),
            dma((2, 3)), dma((2, 3)), dma((2, 2)), dma((2, 2)), dma((2, 3, 2)), dma((2, 3, 2)), dma((2, 2)), dma((2, 2)),
            dma((2,)), dma((2,)), dma((2,)), dma((2,)),
        ],
        compiler_params=pltpu.CompilerParams(collective_id=0, has_side_effects=True, vmem_limit_bytes=60 * 2**20),
    )(load_terms, start_values, reaction_rate)


def solution(mesh):
    spec = P("band", "lane", None)
    return jax.shard_map(
        functools.partial(shards, mesh.shape["lane"], mesh.shape["band"]),
        mesh=mesh,
        in_specs=(spec, spec, spec),
        out_specs=spec,
        check_vma=False,
    )
```
